256 devices in a mesh: vp: 64 (over y, z, core), rep: 4 (over x).
Axes of the slice: x: 4, y: 4, z: 8, core: 2. Of those that a mesh axis runs over, the one named last changes fastest.
Arguments:
- features: bfloat16 [524288, 256], P(('vp', 'rep')), may hold values from -48 to 48
- tile_values: bfloat16 [65536, 128, 128], P(('vp', 'rep')), may hold values from 0 to 0.0014648438
- tile_cols: int32 [65536], P(('vp', 'rep')), may hold values from 0 to 31, as said below
- halo_rows: int32 [256, 4, 4], P(('vp', 'rep')), may hold values from 0 to 15
Outputs:
- scores: bfloat16 [524288, 256], P(('vp', 'rep'))
The draws below stay inside these ranges and needn't reach their ends.
Inputs may be any that keep to these rules, and one draw needn't show every extreme that they name: `tile_cols`: values below 16 name one of the shard's own row blocks; value 16 + o * 4 + j names the j-th block sent by peer o. Every value occurs on every shard.
All inputs are finite; a program needn't handle non-finite values.
Results may differ from the reference program's by a relative error of at most 0.002.
Values may be sent and summed in bfloat16 or wider, within the bound.
A program may use at most 128 MiB of HBM per device.

```python
import math
import jax
import jax.numpy as jnp
from jax import lax

CLASSES = 256
TILE = 128
BLOCKS_DEV = 16
TILES_ROW = 16
HALO_SLOTS = 4
ITERS = 3
SHARDS = 256
VERTICES = 524288
TILES = 65536


def draw_features(key, part):
    scale_key, noise_key, common_key = jax.random.split(key, 3)
    block_count = SHARDS * BLOCKS_DEV
    scales = jnp.exp(jax.random.uniform(scale_key, (block_count, 1, 1), minval=0.0, maxval=math.log(8.0)))
    noise = jnp.clip(jax.random.normal(noise_key, (block_count, TILE, CLASSES)), -6.0, 6.0)
    values = scales * noise
    values = jnp.clip(values, -48.0, 48.0).reshape(block_count * TILE, CLASSES)
    return values.astype(jnp.bfloat16)


def draw_tile_cols(key, part):
    slot_count = BLOCKS_DEV + 4 * HALO_SLOTS
    per_device = BLOCKS_DEV * TILES_ROW
    device_keys = jax.random.split(key, SHARDS)

    def one_device(device_key):
        first_key, second_key = jax.random.split(device_key)
        base_slots = jax.random.randint(first_key, (per_device,), 0, slot_count, dtype=jnp.int32)
        placing = jax.random.permutation(second_key, per_device)
        return base_slots.at[placing[:slot_count]].set(jnp.arange(slot_count, dtype=jnp.int32))
    return jax.vmap(one_device)(device_keys).reshape(-1)


def with_ends(entries, key, least, top_value):
    index_at = [jax.random.randint(jax.random.fold_in(key, axis), (), 0, length) for axis, length in enumerate(entries.shape)]
    main_axis = entries.shape.index(max(entries.shape))
    next_to = index_at[:main_axis] + [(index_at[main_axis] + 1) % entries.shape[main_axis]] + index_at[main_axis + 1:]
    return entries.at[tuple(index_at)].set(least).at[tuple(next_to)].set(top_value)


def levels(key, extent, cuts, least, largest):
    gain, own = 1.0, jax.random.fold_in(key, 6)
    for dim, parts in cuts:
        heights = jnp.exp(jax.random.uniform(jax.random.fold_in(own, dim), (parts,), jnp.float32, least / len(cuts), largest / len(cuts)))
        gain = gain * jnp.repeat(heights, extent[dim] // parts).reshape([-1 if axis == dim else 1 for axis in range(len(extent))])
    return gain


def setup_inputs(seed: int = 0) -> dict:
    seeds = jax.random.split(jax.random.key(seed), 5)
    return {
        "features": draw_features(jax.random.fold_in(seeds[4], 71), 0),
        "tile_values": jnp.clip(0.0014648438 * jax.random.uniform(seeds[1], (TILES, TILE, TILE), jnp.float32) ** levels(seeds[1], (TILES, TILE, TILE), ((0, 256),), -0.2, 0.2), 0.0, 0.0014648438).astype(jnp.bfloat16),
        "tile_cols": draw_tile_cols(jax.random.fold_in(seeds[4], 71), 0),
        "halo_rows": with_ends(jax.random.randint(seeds[3], (SHARDS, 4, HALO_SLOTS), 0, BLOCKS_DEV), jax.random.fold_in(seeds[3], 1), 0, BLOCKS_DEV - 1).astype(jnp.int32),
    }


def reference(features, tile_values, tile_cols, halo_rows):
    nblocks = BLOCKS_DEV
    tiles_dev = BLOCKS_DEV * TILES_ROW
    device_ids = jnp.arange(SHARDS, dtype=jnp.int32)
    slots = tile_cols.reshape(SHARDS, tiles_dev).astype(jnp.int32)
    is_local = slots < nblocks
    halo_slot = jnp.maximum(slots - nblocks, 0)
    offset_slot = (halo_slot // HALO_SLOTS).astype(jnp.int32)
    slot_entry = (halo_slot % HALO_SLOTS).astype(jnp.int32)
    shift_by = jnp.array([1, -1, 4, -4], dtype=jnp.int32)[offset_slot]
    sender = ((device_ids[:, None] - shift_by) % SHARDS).astype(jnp.int32)
    sent_block = halo_rows[sender, offset_slot, slot_entry].astype(jnp.int32)
    source_block = jnp.where(is_local, device_ids[:, None] * nblocks + slots, sender * nblocks + sent_block).astype(jnp.int32)
    source_block = source_block.reshape(SHARDS, nblocks, TILES_ROW)
    tiles = tile_values.reshape(SHARDS, nblocks, TILES_ROW, TILE, TILE)
    teleport_part = 0.1 * features.astype(jnp.float32)
    current = features
    for iteration in range(ITERS):
        blocks = current.reshape(SHARDS * nblocks, TILE, CLASSES)

        def propagate_device(pair):
            tiles_here, sources_here = pair
            gathered = blocks[sources_here]
            return jnp.einsum('rtij,rtjc->ric', tiles_here.astype(jnp.float32), gathered.astype(jnp.float32), precision=lax.Precision.HIGHEST)
        propagated = lax.map(propagate_device, (tiles, source_block)).reshape(VERTICES, CLASSES)
        blended = 0.9 * propagated + teleport_part
        total_mass = lax.optimization_barrier(jnp.sum(blended * blended, axis=0))
        current = (blended / jnp.sqrt(0.05 + total_mass / VERTICES)).astype(jnp.bfloat16)
    return current
```

```python
import jax
import jax.numpy as jnp
from jax import lax
from jax.experimental import pallas as pl
from jax.experimental.pallas import tpu as pltpu
from jax.sharding import PartitionSpec as P

ITERS = 3
TILE = 128
NB = 16
SLOTS = 4
PEERS = 4
KEEP, TELEPORT = 0.9, 0.1
MESH = pl.DeviceIdType.MESH
HALF = 128


def kernel(
    feat_hbm, tiles_hbm, cols, halo, out,
    fbuf, tiles, tab0, tab1, tab2, snd0, snd1, snd2, u1, u2, u3,
    gram, early1, early2, late1, late2,
    load_sem, halo_send, halo_recv, ar_send, ar_recv,
):
    vp, rep = lax.axis_index("vp"), lax.axis_index("rep")
    nvp, nrep = lax.axis_size("vp"), lax.axis_size("rep")
    shards = nvp * nrep
    me = vp * nrep + rep
    vertices = shards * NB * TILE
    plane = vp // 16 * nrep + rep
    column = vp % 16

    def plane_member(i):
        return (i // nrep * 16 + vp % 16, i % nrep)

    def column_member(i):
        return (vp // 16 * 16 + i, rep)

    def peer(o):
        shift = (1, -1, 4, -4)[o]
        d = lax.rem(me + shift + shards, shards)
        return (d // nrep, d % nrep)

    loads = [
        pltpu.make_async_copy(feat_hbm, fbuf, load_sem.at[0]),
        pltpu.make_async_copy(feat_hbm, tab0.at[pl.ds(0, NB)], load_sem.at[1]),
        pltpu.make_async_copy(tiles_hbm, tiles, load_sem.at[2]),
    ]
    for copy in loads:
        copy.start()

    barrier = pltpu.get_barrier_semaphore()
    for o in range(PEERS):
        pl.semaphore_signal(barrier, inc=1, device_id=peer(o), device_id_type=MESH)
    for k in range(1, 16):
        pl.semaphore_signal(
            barrier, inc=1, device_id=plane_member((plane + k) % 16), device_id_type=MESH)
        pl.semaphore_signal(
            barrier, inc=1, device_id=column_member((column + k) % 16), device_id_type=MESH)
    gram[...] = jnp.zeros_like(gram)

    snd, tab = (snd0, snd1, snd2), (tab0, tab1, tab2)

    def halo_copy(step, o, j):
        i = o * SLOTS + j
        return pltpu.make_async_remote_copy(
            src_ref=snd[step].at[i],
            dst_ref=tab[step].at[NB + i],
            send_sem=halo_send.at[step, i],
            recv_sem=halo_recv.at[step, i],
            device_id=peer(o),
            device_id_type=MESH,
        )

    def row_block(table, r):
        total = None
        for p in range(NB // 2):
            t = r * NB + 2 * p
            lhs = jnp.concatenate([tiles[t], tiles[t + 1]], axis=1)
            rhs = jnp.concatenate([table[cols[t]], table[cols[t + 1]]], axis=0)
            term = jnp.dot(lhs, rhs, preferred_element_type=jnp.float32)
            total = term if total is None else total + term
        return total

    def fold(x):
        return jnp.sum(x.reshape(NB, 8, x.shape[-1]), axis=0)

    loads[0].wait()
    for j in range(SLOTS):
        for o in range(PEERS):
            snd0[o * SLOTS + j] = fbuf[halo[0, o, j]]
    pl.semaphore_wait(barrier, PEERS + 30)
    for j in range(SLOTS):
        for o in range(PEERS):
            halo_copy(0, o, j).start()
    loads[1].wait()
    loads[2].wait()

    def wait_halo(step):
        for o in range(PEERS):
            for j in range(SLOTS):
                halo_copy(step, o, j).wait_recv()

    def send_pass(step):
        def body(j, _):
            for o in range(PEERS):
                snd[step][o * SLOTS + j] = row_block(tab[step - 1], halo[0, o, j]).astype(jnp.bfloat16)
                halo_copy(step, o, j).start()
            return 0

        lax.fori_loop(0, SLOTS, body, 0)

    def own_pass(step, keep, others, first):
        def body(q, _):
            for part in range(4):
                r = q * 4 + part
                u = row_block(tab[step - 1], r)
                keep[r] = u
                if step < ITERS:
                    tab[step][r] = u.astype(jnp.bfloat16)
                for i, other in enumerate(others):
                    gram[first + i] += fold(other[r].astype(jnp.float32) * u)
                gram[first + len(others)] += fold(u * u)
            return 0

        lax.fori_loop(0, 4, body, 0)

    def pack(buf, mine, first, count):
        for i in range(count):
            row = jnp.sum(gram[first + i], axis=0, keepdims=True)
            for h in range(2):
                buf[mine, pl.ds(2 * i + h, 1), :] = row[:, h * HALF:(h + 1) * HALF]

    def stage(number, buf, mine, member):
        copies = []
        for k in range(1, 16):
            copies.append(pltpu.make_async_remote_copy(
                src_ref=buf.at[mine],
                dst_ref=buf.at[mine],
                send_sem=ar_send.at[number, k - 1],
                recv_sem=ar_recv.at[number, k - 1],
                device_id=member((mine + k) % 16),
                device_id_type=MESH,
            ))
        return copies

    def total_of(buf):
        total = buf[0]
        for i in range(1, 16):
            total = total + buf[i]
        return total

    wait_halo(0)
    send_pass(1)
    def ff_body(r, _):
        f = fbuf[r].astype(jnp.float32)
        gram[0] += fold(f * f)
        return 0
    lax.fori_loop(0, NB, ff_body, 0)
    own_pass(1, u1, (fbuf,), 1)
    wait_halo(1)
    send_pass(2)
    own_pass(2, u2, (fbuf, u1), 3)
    early1[plane, pl.ds(12, 4), :] = jnp.zeros((4, HALF), jnp.float32)
    pack(early1, plane, 0, 6)
    early_a = stage(0, early1, plane, plane_member)
    for copy in early_a:
        copy.start()
    wait_halo(2)
    for copy in early_a:
        copy.wait_recv()
    early2[column] = total_of(early1)
    early_b = stage(1, early2, column, column_member)
    for copy in early_b:
        copy.start()
    own_pass(3, u3, (fbuf, u1, u2), 6)
    pack(late1, plane, 6, 4)
    late_a = stage(2, late1, plane, plane_member)
    for copy in late_a:
        copy.start()
    for copy in early_b:
        copy.wait_recv()
    early = total_of(early2)
    for copy in late_a:
        copy.wait_recv()
    late2[column] = total_of(late1)
    late_b = stage(3, late2, column, column_member)
    for copy in late_b:
        copy.start()

    def row(block, i):
        return jnp.concatenate([block[2 * i:2 * i + 1], block[2 * i + 1:2 * i + 2]], axis=1)

    a, b = KEEP, TELEPORT
    ff, f1, g11, f2, g12, g22 = (row(early, i) for i in range(6))
    mass1 = a * a * g11 + 2 * a * b * f1 + b * b * ff
    s1 = 1.0 / jnp.sqrt(0.05 + mass1 / vertices)
    w22 = a * a * g22 + 2 * a * b * g12 + b * b * g11
    w2f = a * f2 + b * f1
    mass2 = (a * s1) * (a * s1) * w22 + 2 * a * b * s1 * w2f + b * b * ff
    s2 = 1.0 / jnp.sqrt(0.05 + mass2 / vertices)
    c3 = a * a * a * s1 * s2
    c2 = a * a * b * s1 * s2
    c1 = a * b * s2

    def blend(r, _):
        u3[r] = c3 * u3[r] + c2 * u2[r] + c1 * u1[r] + b * fbuf[r].astype(jnp.float32)
        return 0

    lax.fori_loop(0, NB, blend, 0)
    for copy in late_b:
        copy.wait_recv()
    late = total_of(late2)
    f3, g13, g23, g33 = (row(late, i) for i in range(4))
    mass3 = (
        c3 * c3 * g33 + c2 * c2 * g22 + c1 * c1 * g11 + b * b * ff
        + 2 * (c3 * c2 * g23 + c3 * c1 * g13 + c2 * c1 * g12)
        + 2 * b * (c3 * f3 + c2 * f2 + c1 * f1)
    )
    s3 = 1.0 / jnp.sqrt(0.05 + mass3 / vertices)

    def finish(r, _):
        out[r] = (u3[r] * s3).astype(jnp.bfloat16)
        return 0

    lax.fori_loop(0, NB, finish, 0)

    for step in range(ITERS):
        for o in range(PEERS):
            for j in range(SLOTS):
                halo_copy(step, o, j).wait_send()
    for copy in early_a + early_b + late_a + late_b:
        copy.wait_send()


def local(features, tile_values, tile_cols, halo_rows):
    classes = features.shape[1]
    rows = (NB, TILE, classes)
    anywhere = pl.BlockSpec(memory_space=pl.ANY)
    scalars = pl.BlockSpec(memory_space=pltpu.SMEM)
    table = pltpu.VMEM((2 * NB, TILE, classes), jnp.bfloat16)
    blocks = pltpu.VMEM(rows, jnp.bfloat16)
    wide = pltpu.VMEM(rows, jnp.float32)
    scores = pl.pallas_call(
        kernel,
        out_shape=jax.ShapeDtypeStruct(rows, jnp.bfloat16),
        in_specs=[anywhere, anywhere, scalars, scalars],
        out_specs=pl.BlockSpec(memory_space=pltpu.VMEM),
        scratch_shapes=[
            blocks,
            pltpu.VMEM(tile_values.shape, jnp.bfloat16),
            table, table, table,
            blocks, blocks, blocks,
            wide, wide, wide,
            pltpu.VMEM((10, 8, classes), jnp.float32),
            pltpu.VMEM((16, 16, HALF), jnp.float32),
            pltpu.VMEM((16, 16, HALF), jnp.float32),
            pltpu.VMEM((16, 8, HALF), jnp.float32),
            pltpu.VMEM((16, 8, HALF), jnp.float32),
            pltpu.SemaphoreType.DMA((3,)),
            pltpu.SemaphoreType.DMA((ITERS, NB)),
            pltpu.SemaphoreType.DMA((ITERS, NB)),
            pltpu.SemaphoreType.DMA((4, 15)),
            pltpu.SemaphoreType.DMA((4, 15)),
        ],
        compiler_params=pltpu.CompilerParams(
            collective_id=0, has_side_effects=True, vmem_limit_bytes=40 * 1024 * 1024
        ),
        name="propagate",
    )(features.reshape(rows), tile_values, tile_cols, halo_rows)
    return scores.reshape(features.shape)


def solution(mesh):
    return jax.shard_map(
        local,
        mesh=mesh,
        in_specs=(
            P(("vp", "rep"), None),
            P(("vp", "rep"), None, None),
            P(("vp", "rep")),
            P(("vp", "rep"), None, None),
        ),
        out_specs=P(("vp", "rep"), None),
        check_vma=False,
    )
```

```python
import jax
import jax.numpy as jnp
from jax import lax
from jax.experimental import pallas as pl
from jax.experimental.pallas import tpu as pltpu
from jax.sharding import PartitionSpec as P

ITERS = 3
TILE = 128
NB = 16
SLOTS = 4
PEERS = 4
KEEP, TELEPORT = 0.9, 0.1
MESH = pl.DeviceIdType.MESH
HALF = 128


def kernel(
    feat_hbm, tiles_hbm, cols_hbm, halo_hbm, out,
    cols, halo, fbuf, tiles, tab0, tab1, tab2, snd0, snd1, snd2, u1, u2, u3,
    gram, early1, early2, late1, late2,
    load_sem, halo_send, halo_recv, ar_send, ar_recv,
):
    vp, rep = lax.axis_index("vp"), lax.axis_index("rep")
    nvp, nrep = lax.axis_size("vp"), lax.axis_size("rep")
    shards = nvp * nrep
    me = vp * nrep + rep
    vertices = shards * NB * TILE
    plane = vp // 16 * nrep + rep
    column = vp % 16

    def plane_member(i):
        return (i // nrep * 16 + vp % 16, i % nrep)

    def column_member(i):
        return (vp // 16 * 16 + i, rep)

    core = vp % 2

    def peer(o):
        shift = (1 - o % 2 * 2) * (1 + o // 2 * 3)
        d = lax.rem(me + shift + shards, shards)
        return (d // nrep, d % nrep)

    leading, staying, trailing, across = 1 - core, 2 + core, core, 3 - core

    loads = [
        pltpu.make_async_copy(feat_hbm, fbuf, load_sem.at[0]),
        pltpu.make_async_copy(feat_hbm, tab0.at[pl.ds(0, NB)], load_sem.at[1]),
        pltpu.make_async_copy(tiles_hbm, tiles, load_sem.at[2]),
        pltpu.make_async_copy(cols_hbm, cols, load_sem.at[3]),
        pltpu.make_async_copy(halo_hbm, halo, load_sem.at[4]),
    ]
    for i in (4, 0, 3, 1, 2):
        loads[i].start()

    barrier = pltpu.get_barrier_semaphore()
    for o in range(PEERS):
        pl.semaphore_signal(barrier, inc=1, device_id=peer(o), device_id_type=MESH)
    for k in range(1, 16):
        pl.semaphore_signal(
            barrier, inc=1, device_id=plane_member((plane + k) % 16), device_id_type=MESH)
        pl.semaphore_signal(
            barrier, inc=1, device_id=column_member((column + k) % 16), device_id_type=MESH)
    gram[...] = jnp.zeros_like(gram)

    snd, tab = (snd0, snd1, snd2), (tab0, tab1, tab2)

    def halo_copy(step, o, j):
        i = o * SLOTS + j
        return pltpu.make_async_remote_copy(
            src_ref=snd[step].at[i],
            dst_ref=tab[step].at[NB + i],
            send_sem=halo_send.at[step, i],
            recv_sem=halo_recv.at[step, i],
            device_id=peer(o),
            device_id_type=MESH,
        )

    def row_block(table, r):
        total = None
        for p in range(NB // 2):
            t = r * NB + 2 * p
            lhs = jnp.concatenate([tiles[t], tiles[t + 1]], axis=1)
            rhs = jnp.concatenate([table[cols[t]], table[cols[t + 1]]], axis=0)
            term = jnp.dot(lhs, rhs, preferred_element_type=jnp.float32)
            total = term if total is None else total + term
        return total

    def fold(x):
        return jnp.sum(x.reshape(NB, 8, x.shape[-1]), axis=0)

    loads[4].wait()
    loads[0].wait()
    for j in range(SLOTS):
        for o in range(PEERS):
            snd0[o * SLOTS + j] = fbuf[halo[0, o, j]]
    pl.semaphore_wait(barrier, PEERS + 30)
    for o in (leading, staying):
        for j in range(SLOTS):
            halo_copy(0, o, j).start()
    for j in range(SLOTS):
        for o in (trailing, across):
            halo_copy(0, o, j).start()
    for i in (1, 2, 3):
        loads[i].wait()

    def wait_halo(step):
        for o in range(PEERS):
            for j in range(SLOTS):
                halo_copy(step, o, j).wait_recv()

    def send_pass(step):
        def send(o, j):
            i = o * SLOTS + j
            snd[step][i] = row_block(tab[step - 1], halo[0, o, j]).astype(jnp.bfloat16)
            halo_copy(step, o, j).start()

        def one(o):
            def body(j, _):
                send(o, j)
                return 0
            lax.fori_loop(0, SLOTS, body, 0)

        def two(j, _):
            send(trailing, j)
            send(across, j)
            return 0

        one(leading)
        one(staying)
        lax.fori_loop(0, SLOTS, two, 0)

    def own_pass(step, keep, others, first):
        def body(q, _):
            for part in range(4):
                r = q * 4 + part
                u = row_block(tab[step - 1], r)
                keep[r] = u
                if step < ITERS:
                    tab[step][r] = u.astype(jnp.bfloat16)
                for i, other in enumerate(others):
                    gram[first + i] += fold(other[r].astype(jnp.float32) * u)
                gram[first + len(others)] += fold(u * u)
            return 0

        lax.fori_loop(0, 4, body, 0)

    def pack(buf, mine, first, count):
        for i in range(count):
            row = jnp.sum(gram[first + i], axis=0, keepdims=True)
            for h in range(2):
                buf[mine, pl.ds(2 * i + h, 1), :] = row[:, h * HALF:(h + 1) * HALF]

    def stage(number, buf, mine, member):
        copies = []
        for k in range(1, 16):
            copies.append(pltpu.make_async_remote_copy(
                src_ref=buf.at[mine],
                dst_ref=buf.at[mine],
                send_sem=ar_send.at[number, k - 1],
                recv_sem=ar_recv.at[number, k - 1],
                device_id=member((mine + k) % 16),
                device_id_type=MESH,
            ))
        return copies

    def total_of(buf):
        total = buf[0]
        for i in range(1, 16):
            total = total + buf[i]
        return total

    wait_halo(0)
    send_pass(1)
    def ff_body(r, _):
        f = fbuf[r].astype(jnp.float32)
        gram[0] += fold(f * f)
        return 0
    lax.fori_loop(0, NB, ff_body, 0)
    own_pass(1, u1, (fbuf,), 1)
    wait_halo(1)
    send_pass(2)
    own_pass(2, u2, (fbuf, u1), 3)
    early1[plane, pl.ds(12, 4), :] = jnp.zeros((4, HALF), jnp.float32)
    pack(early1, plane, 0, 6)
    early_a = stage(0, early1, plane, plane_member)
    for copy in early_a:
        copy.start()
    wait_halo(2)
    for copy in early_a:
        copy.wait_recv()
    early2[column] = total_of(early1)
    early_b = stage(1, early2, column, column_member)
    for copy in early_b:
        copy.start()
    own_pass(3, u3, (fbuf, u1, u2), 6)
    pack(late1, plane, 6, 4)
    late_a = stage(2, late1, plane, plane_member)
    for copy in late_a:
        copy.start()
    for copy in early_b:
        copy.wait_recv()
    early = total_of(early2)
    for copy in late_a:
        copy.wait_recv()
    late2[column] = total_of(late1)
    late_b = stage(3, late2, column, column_member)
    for copy in late_b:
        copy.start()

    def row(block, i):
        return jnp.concatenate([block[2 * i:2 * i + 1], block[2 * i + 1:2 * i + 2]], axis=1)

    a, b = KEEP, TELEPORT
    ff, f1, g11, f2, g12, g22 = (row(early, i) for i in range(6))
    mass1 = a * a * g11 + 2 * a * b * f1 + b * b * ff
    s1 = 1.0 / jnp.sqrt(0.05 + mass1 / vertices)
    w22 = a * a * g22 + 2 * a * b * g12 + b * b * g11
    w2f = a * f2 + b * f1
    mass2 = (a * s1) * (a * s1) * w22 + 2 * a * b * s1 * w2f + b * b * ff
    s2 = 1.0 / jnp.sqrt(0.05 + mass2 / vertices)
    c3 = a * a * a * s1 * s2
    c2 = a * a * b * s1 * s2
    c1 = a * b * s2

    def blend(r, _):
        u3[r] = c3 * u3[r] + c2 * u2[r] + c1 * u1[r] + b * fbuf[r].astype(jnp.float32)
        return 0

    lax.fori_loop(0, NB, blend, 0)
    for copy in late_b:
        copy.wait_recv()
    late = total_of(late2)
    f3, g13, g23, g33 = (row(late, i) for i in range(4))
    mass3 = (
        c3 * c3 * g33 + c2 * c2 * g22 + c1 * c1 * g11 + b * b * ff
        + 2 * (c3 * c2 * g23 + c3 * c1 * g13 + c2 * c1 * g12)
        + 2 * b * (c3 * f3 + c2 * f2 + c1 * f1)
    )
    s3 = 1.0 / jnp.sqrt(0.05 + mass3 / vertices)

    def finish(r, _):
        out[r] = (u3[r] * s3).astype(jnp.bfloat16)
        return 0

    lax.fori_loop(0, NB, finish, 0)

    for step in range(ITERS):
        for j in range(SLOTS):
            for o in range(PEERS):
                halo_copy(step, o, j).wait_send()
    for copy in early_a + early_b + late_a + late_b:
        copy.wait_send()


def local(features, tile_values, tile_cols, halo_rows):
    classes = features.shape[1]
    rows = (NB, TILE, classes)
    anywhere = pl.BlockSpec(memory_space=pltpu.HBM)
    table = pltpu.VMEM((2 * NB, TILE, classes), jnp.bfloat16)
    blocks = pltpu.VMEM(rows, jnp.bfloat16)
    wide = pltpu.VMEM(rows, jnp.float32)
    inputs = [
        pltpu.with_memory_space_constraint(v, pltpu.HBM)
        for v in (features.reshape(rows), tile_values, tile_cols, halo_rows)
    ]
    scores = pl.pallas_call(
        kernel,
        out_shape=jax.ShapeDtypeStruct(rows, jnp.bfloat16),
        in_specs=[anywhere] * 4,
        out_specs=pl.BlockSpec(memory_space=pltpu.VMEM),
        scratch_shapes=[
            pltpu.SMEM(tile_cols.shape, jnp.int32),
            pltpu.SMEM(halo_rows.shape, jnp.int32),
            blocks,
            pltpu.VMEM(tile_values.shape, jnp.bfloat16),
            table, table, table,
            blocks, blocks, blocks,
            wide, wide, wide,
            pltpu.VMEM((10, 8, classes), jnp.float32),
            pltpu.VMEM((16, 16, HALF), jnp.float32),
            pltpu.VMEM((16, 16, HALF), jnp.float32),
            pltpu.VMEM((16, 8, HALF), jnp.float32),
            pltpu.VMEM((16, 8, HALF), jnp.float32),
            pltpu.SemaphoreType.DMA((5,)),
            pltpu.SemaphoreType.DMA((ITERS, NB)),
            pltpu.SemaphoreType.DMA((ITERS, NB)),
            pltpu.SemaphoreType.DMA((4, 15)),
            pltpu.SemaphoreType.DMA((4, 15)),
        ],
        compiler_params=pltpu.CompilerParams(
            collective_id=0, has_side_effects=True, vmem_limit_bytes=40 * 1024 * 1024
        ),
        name="propagate",
    )(*inputs)
    return scores.reshape(features.shape)


def solution(mesh):
    return jax.shard_map(
        local,
        mesh=mesh,
        in_specs=(
            P(("vp", "rep"), None),
            P(("vp", "rep"), None, None),
            P(("vp", "rep")),
            P(("vp", "rep"), None, None),
        ),
        out_specs=P(("vp", "rep"), None),
        check_vma=False,
    )
```

```python
import jax
import jax.numpy as jnp
from jax import lax
from jax.experimental import pallas as pl
from jax.experimental.pallas import tpu as pltpu
from jax.sharding import PartitionSpec as P

ITERS = 3
TILE = 128
NB = 16
SLOTS = 4
PEERS = 4
KEEP, TELEPORT = 0.9, 0.1
MESH = pl.DeviceIdType.MESH
HALF = 128


def kernel(
    feat_hbm, tiles_hbm, cols_hbm, halo_hbm, out,
    cols, halo, fbuf, tiles, tab0, tab1, tab2, snd0, snd1, snd2, u1, u2, u3,
    gram, early1, early2, late1, late2,
    load_sem, halo_send, halo_recv, ar_send, ar_recv,
):
    vp, rep = lax.axis_index("vp"), lax.axis_index("rep")
    nvp, nrep = lax.axis_size("vp"), lax.axis_size("rep")
    shards = nvp * nrep
    me = vp * nrep + rep
    vertices = shards * NB * TILE
    plane = vp // 16 * nrep + rep
    column = vp % 16

    def plane_member(i):
        return (i // nrep * 16 + vp % 16, i % nrep)

    def column_member(i):
        return (vp // 16 * 16 + i, rep)

    core = vp % 2

    def peer(o):
        shift = (1 - o % 2 * 2) * (1 + o // 2 * 3)
        d = lax.rem(me + shift + shards, shards)
        return (d // nrep, d % nrep)

    leading, across, trailing, staying = 1 - core, 3 - core, core, 2 + core

    loads = [
        pltpu.make_async_copy(feat_hbm, fbuf, load_sem.at[0]),
        pltpu.make_async_copy(feat_hbm, tab0.at[pl.ds(0, NB)], load_sem.at[1]),
        pltpu.make_async_copy(tiles_hbm, tiles, load_sem.at[2]),
        pltpu.make_async_copy(cols_hbm, cols, load_sem.at[3]),
        pltpu.make_async_copy(halo_hbm, halo, load_sem.at[4]),
    ]
    for i in (4, 0, 3, 1, 2):
        loads[i].start()

    barrier = pltpu.get_barrier_semaphore()
    for o in range(PEERS):
        pl.semaphore_signal(barrier, inc=1, device_id=peer(o), device_id_type=MESH)
    for k in range(1, 16):
        pl.semaphore_signal(
            barrier, inc=1, device_id=plane_member((plane + k) % 16), device_id_type=MESH)
        pl.semaphore_signal(
            barrier, inc=1, device_id=column_member((column + k) % 16), device_id_type=MESH)
    gram[...] = jnp.zeros_like(gram)

    snd, tab = (snd0, snd1, snd2), (tab0, tab1, tab2)

    def halo_copy(step, o, j):
        i = o * SLOTS + j
        return pltpu.make_async_remote_copy(
            src_ref=snd[step].at[i],
            dst_ref=tab[step].at[NB + i],
            send_sem=halo_send.at[step, i],
            recv_sem=halo_recv.at[step, i],
            device_id=peer(o),
            device_id_type=MESH,
        )

    def row_block(table, r):
        total = None
        for p in range(NB // 2):
            t = r * NB + 2 * p
            lhs = jnp.concatenate([tiles[t], tiles[t + 1]], axis=1)
            rhs = jnp.concatenate([table[cols[t]], table[cols[t + 1]]], axis=0)
            term = jnp.dot(lhs, rhs, preferred_element_type=jnp.float32)
            total = term if total is None else total + term
        return total

    def fold(x):
        return jnp.sum(x.reshape(NB, 8, x.shape[-1]), axis=0)

    loads[4].wait()
    loads[0].wait()
    for j in range(SLOTS):
        for o in range(PEERS):
            snd0[o * SLOTS + j] = fbuf[halo[0, o, j]]
    pl.semaphore_wait(barrier, PEERS + 30)
    for o in (leading, across, trailing, staying):
        for j in range(SLOTS):
            halo_copy(0, o, j).start()
    for i in (1, 2, 3):
        loads[i].wait()

    def wait_halo(step):
        for o in range(PEERS):
            for j in range(SLOTS):
                halo_copy(step, o, j).wait_recv()

    def send_pass(step):
        def send(o, j):
            i = o * SLOTS + j
            snd[step][i] = row_block(tab[step - 1], halo[0, o, j]).astype(jnp.bfloat16)
            halo_copy(step, o, j).start()

        def one(o):
            def body(j, _):
                send(o, j)
                return 0
            lax.fori_loop(0, SLOTS, body, 0)

        for o in (leading, across, trailing, staying):
            one(o)

    def own_pass(step, keep, others, first):
        def body(q, _):
            for part in range(4):
                r = q * 4 + part
                u = row_block(tab[step - 1], r)
                keep[r] = u
                if step < ITERS:
                    tab[step][r] = u.astype(jnp.bfloat16)
                for i, other in enumerate(others):
                    gram[first + i] += fold(other[r].astype(jnp.float32) * u)
                gram[first + len(others)] += fold(u * u)
            return 0

        lax.fori_loop(0, 4, body, 0)

    def pack(buf, mine, first, count):
        for i in range(count):
            row = jnp.sum(gram[first + i], axis=0, keepdims=True)
            for h in range(2):
                buf[mine, pl.ds(2 * i + h, 1), :] = row[:, h * HALF:(h + 1) * HALF]

    def stage(number, buf, mine, member):
        copies = []
        for k in range(1, 16):
            copies.append(pltpu.make_async_remote_copy(
                src_ref=buf.at[mine],
                dst_ref=buf.at[mine],
                send_sem=ar_send.at[number, k - 1],
                recv_sem=ar_recv.at[number, k - 1],
                device_id=member((mine + k) % 16),
                device_id_type=MESH,
            ))
        return copies

    def total_of(buf):
        total = buf[0]
        for i in range(1, 16):
            total = total + buf[i]
        return total

    wait_halo(0)
    send_pass(1)
    def ff_body(r, _):
        f = fbuf[r].astype(jnp.float32)
        gram[0] += fold(f * f)
        return 0
    lax.fori_loop(0, NB, ff_body, 0)
    own_pass(1, u1, (fbuf,), 1)
    wait_halo(1)
    send_pass(2)
    own_pass(2, u2, (fbuf, u1), 3)
    early1[plane, pl.ds(12, 4), :] = jnp.zeros((4, HALF), jnp.float32)
    pack(early1, plane, 0, 6)
    early_a = stage(0, early1, plane, plane_member)
    for copy in early_a:
        copy.start()
    wait_halo(2)
    own_pass(3, u3, (fbuf, u1, u2), 6)
    pack(late1, plane, 6, 4)
    late_a = stage(2, late1, plane, plane_member)
    for copy in late_a:
        copy.start()
    for copy in early_a:
        copy.wait_recv()
    early2[column] = total_of(early1)
    early_b = stage(1, early2, column, column_member)
    for copy in early_b:
        copy.start()
    for copy in early_b:
        copy.wait_recv()
    early = total_of(early2)

    def row(block, i):
        return jnp.concatenate([block[2 * i:2 * i + 1], block[2 * i + 1:2 * i + 2]], axis=1)

    def scale_of(mass):
        return 1.0 / jnp.sqrt(0.05 + mass / vertices)

    a, b = KEEP, TELEPORT
    ff, f1, g11, f2, g12, g22 = (row(early, i) for i in range(6))
    s1 = scale_of(a * a * g11 + 2 * a * b * f1 + b * b * ff)
    w22 = a * a * g22 + 2 * a * b * g12 + b * b * g11
    w2f = a * f2 + b * f1
    s2 = scale_of((a * s1) * (a * s1) * w22 + 2 * a * b * s1 * w2f + b * b * ff)
    c3 = a * a * a * s1 * s2
    c2 = a * a * b * s1 * s2
    c1 = a * b * s2

    for copy in late_a:
        copy.wait_recv()
    part = total_of(late1)
    f3, g13, g23, g33 = (row(part, i) for i in range(4))
    part = c3 * c3 * g33 + 2 * c3 * (c2 * g23 + c1 * g13 + b * f3)
    for h in range(2):
        late2[column, pl.ds(h, 1), :] = part[:, h * HALF:(h + 1) * HALF]
    late_b = stage(3, late2, column, column_member)
    for copy in late_b:
        copy.start()
    known = (
        c2 * c2 * g22 + c1 * c1 * g11 + b * b * ff
        + 2 * c2 * (c1 * g12 + b * f2) + 2 * b * c1 * f1
    )

    def blend(r, _):
        u3[r] = c3 * u3[r] + c2 * u2[r] + c1 * u1[r] + b * fbuf[r].astype(jnp.float32)
        return 0

    lax.fori_loop(0, NB, blend, 0)
    for copy in late_b:
        copy.wait_recv()
    s3 = scale_of(known + row(total_of(late2), 0))

    def finish(r, _):
        out[r] = (u3[r] * s3).astype(jnp.bfloat16)
        return 0

    lax.fori_loop(0, NB, finish, 0)

    for step in range(ITERS):
        for j in range(SLOTS):
            for o in range(PEERS):
                halo_copy(step, o, j).wait_send()
    for copy in early_a + early_b + late_a + late_b:
        copy.wait_send()


def local(features, tile_values, tile_cols, halo_rows):
    classes = features.shape[1]
    rows = (NB, TILE, classes)
    anywhere = pl.BlockSpec(memory_space=pltpu.HBM)
    table = pltpu.VMEM((2 * NB, TILE, classes), jnp.bfloat16)
    blocks = pltpu.VMEM(rows, jnp.bfloat16)
    wide = pltpu.VMEM(rows, jnp.float32)
    inputs = [
        pltpu.with_memory_space_constraint(v, pltpu.HBM)
        for v in (features.reshape(rows), tile_values, tile_cols, halo_rows)
    ]
    scores = pl.pallas_call(
        kernel,
        out_shape=jax.ShapeDtypeStruct(rows, jnp.bfloat16),
        in_specs=[anywhere] * 4,
        out_specs=pl.BlockSpec(memory_space=pltpu.VMEM),
        scratch_shapes=[
            pltpu.SMEM(tile_cols.shape, jnp.int32),
            pltpu.SMEM(halo_rows.shape, jnp.int32),
            blocks,
            pltpu.VMEM(tile_values.shape, jnp.bfloat16),
            table, table, table,
            blocks, blocks, blocks,
            wide, wide, wide,
            pltpu.VMEM((10, 8, classes), jnp.float32),
            pltpu.VMEM((16, 16, HALF), jnp.float32),
            pltpu.VMEM((16, 16, HALF), jnp.float32),
            pltpu.VMEM((16, 8, HALF), jnp.float32),
            pltpu.VMEM((16, 2, HALF), jnp.float32),
            pltpu.SemaphoreType.DMA((5,)),
            pltpu.SemaphoreType.DMA((ITERS, NB)),
            pltpu.SemaphoreType.DMA((ITERS, NB)),
            pltpu.SemaphoreType.DMA((4, 15)),
            pltpu.SemaphoreType.DMA((4, 15)),
        ],
        compiler_params=pltpu.CompilerParams(
            collective_id=0, has_side_effects=True, vmem_limit_bytes=40 * 1024 * 1024
        ),
        name="propagate",
    )(*inputs)
    return scores.reshape(features.shape)


def solution(mesh):
    return jax.shard_map(
        local,
        mesh=mesh,
        in_specs=(
            P(("vp", "rep"), None),
            P(("vp", "rep"), None, None),
            P(("vp", "rep")),
            P(("vp", "rep"), None, None),
        ),
        out_specs=P(("vp", "rep"), None),
        check_vma=False,
    )
```

```python
import jax
import jax.numpy as jnp
from jax import lax
from jax.experimental import pallas as pl
from jax.experimental.pallas import tpu as pltpu
from jax.sharding import PartitionSpec as P

ITERS = 3
TILE = 128
NB = 16
SLOTS = 4
PEERS = 4
KEEP, TELEPORT = 0.9, 0.1
MESH = pl.DeviceIdType.MESH
HALF = 128


def kernel(
    feat_hbm, tiles_hbm, cols_hbm, halo_hbm, out,
    cols, halo, fbuf, tiles, tab0, tab1, tab2, snd0, snd1, snd2, u1, u2, last,
    gram, early1, early2, late1, late2,
    load_sem, halo_send, halo_recv, ar_send, ar_recv,
):
    vp, rep = lax.axis_index("vp"), lax.axis_index("rep")
    nvp, nrep = lax.axis_size("vp"), lax.axis_size("rep")
    shards = nvp * nrep
    me = vp * nrep + rep
    vertices = shards * NB * TILE
    plane = vp // 16 * nrep + rep
    column = vp % 16

    def plane_member(i):
        return (i // nrep * 16 + vp % 16, i % nrep)

    def column_member(i):
        return (vp // 16 * 16 + i, rep)

    core = vp % 2

    def peer(o):
        shift = (1 - o % 2 * 2) * (1 + o // 2 * 3)
        d = lax.rem(me + shift + shards, shards)
        return (d // nrep, d % nrep)

    leading, trailing, across, staying = 1 - core, core, 3 - core, 2 + core

    loads = [
        pltpu.make_async_copy(feat_hbm, fbuf, load_sem.at[0]),
        pltpu.make_async_copy(feat_hbm, tab0.at[pl.ds(0, NB)], load_sem.at[1]),
        pltpu.make_async_copy(tiles_hbm, tiles, load_sem.at[2]),
        pltpu.make_async_copy(cols_hbm, cols, load_sem.at[3]),
        pltpu.make_async_copy(halo_hbm, halo, load_sem.at[4]),
    ]
    for i in (4, 0, 3, 1, 2):
        loads[i].start()

    barrier = pltpu.get_barrier_semaphore()
    for o in range(PEERS):
        pl.semaphore_signal(barrier, inc=1, device_id=peer(o), device_id_type=MESH)
    for k in range(1, 16):
        pl.semaphore_signal(
            barrier, inc=1, device_id=plane_member((plane + k) % 16), device_id_type=MESH)
        pl.semaphore_signal(
            barrier, inc=1, device_id=column_member((column + k) % 16), device_id_type=MESH)
    gram[...] = jnp.zeros_like(gram)

    snd, tab = (snd0, snd1, snd2), (tab0, tab1, tab2)

    def halo_copy(step, o, j):
        i = o * SLOTS + j
        return pltpu.make_async_remote_copy(
            src_ref=snd[step].at[i],
            dst_ref=tab[step].at[NB + i],
            send_sem=halo_send.at[step, i],
            recv_sem=halo_recv.at[step, i],
            device_id=peer(o),
            device_id_type=MESH,
        )

    def row_block(table, r):
        total = None
        for p in range(NB // 2):
            t = r * NB + 2 * p
            lhs = jnp.concatenate([tiles[t], tiles[t + 1]], axis=1)
            rhs = jnp.concatenate([table[cols[t]], table[cols[t + 1]]], axis=0)
            term = jnp.dot(lhs, rhs, preferred_element_type=jnp.float32)
            total = term if total is None else total + term
        return total

    def fold(x):
        return jnp.sum(x.reshape(NB, 8, x.shape[-1]), axis=0)

    loads[4].wait()
    loads[0].wait()
    for j in range(SLOTS):
        for o in range(PEERS):
            snd0[o * SLOTS + j] = fbuf[halo[0, o, j]]
    pl.semaphore_wait(barrier, PEERS + 30)
    for o in (leading, trailing, across, staying):
        for j in range(SLOTS):
            halo_copy(0, o, j).start()
    for i in (1, 2, 3):
        loads[i].wait()

    def wait_halo(step):
        for o in range(PEERS):
            for j in range(SLOTS):
                halo_copy(step, o, j).wait_recv()

    def send_pass(step):
        def send(o, j):
            i = o * SLOTS + j
            snd[step][i] = row_block(tab[step - 1], halo[0, o, j]).astype(jnp.bfloat16)
            halo_copy(step, o, j).start()

        def one(o):
            def body(j, _):
                send(o, j)
                return 0
            lax.fori_loop(0, SLOTS, body, 0)

        for o in (leading, trailing, across, staying):
            one(o)

    def each_block(work):
        def body(q, _):
            for part in range(4):
                work(q * 4 + part)
            return 0

        lax.fori_loop(0, NB // 4, body, 0)

    def wide_f(r):
        return fbuf[r].astype(jnp.float32)

    def own_first(r):
        u = row_block(tab0, r)
        u1[r] = u
        tab1[r] = u.astype(jnp.bfloat16)
        f = wide_f(r)
        gram[0] += fold(f * f)
        gram[1] += fold(f * u)
        gram[2] += fold(u * u)

    def own_second(r):
        u = row_block(tab1, r)
        u2[r] = u
        tab2[r] = u.astype(jnp.bfloat16)
        w = KEEP * u + TELEPORT * u1[r]
        gram[3] += fold(w * w)
        gram[4] += fold(w * wide_f(r))

    def own_third(r):
        w = KEEP * row_block(tab2, r) + TELEPORT * u2[r]
        last[r] = w
        gram[5] += fold(w * w)
        gram[6] += fold(w * u1[r])
        gram[7] += fold(w * wide_f(r))

    def pack(buf, mine, first, count):
        for i in range(count):
            row = jnp.sum(gram[first + i], axis=0, keepdims=True)
            for h in range(2):
                buf[mine, pl.ds(2 * i + h, 1), :] = row[:, h * HALF:(h + 1) * HALF]

    def stage(number, buf, mine, member):
        copies = []
        for k in range(1, 16):
            copies.append(pltpu.make_async_remote_copy(
                src_ref=buf.at[mine],
                dst_ref=buf.at[mine],
                send_sem=ar_send.at[number, k - 1],
                recv_sem=ar_recv.at[number, k - 1],
                device_id=member((mine + k) % 16),
                device_id_type=MESH,
            ))
        return copies

    def total_of(buf):
        total = buf[0]
        for i in range(1, 16):
            total = total + buf[i]
        return total

    wait_halo(0)
    send_pass(1)
    each_block(own_first)
    wait_halo(1)
    send_pass(2)
    each_block(own_second)
    pack(early1, plane, 0, 5)
    early_a = stage(0, early1, plane, plane_member)
    for copy in early_a:
        copy.start()
    wait_halo(2)
    each_block(own_third)
    pack(late1, plane, 5, 3)
    late_a = stage(2, late1, plane, plane_member)
    for copy in late_a:
        copy.start()
    for copy in early_a:
        copy.wait_recv()
    early2[column] = total_of(early1)
    early_b = stage(1, early2, column, column_member)
    for copy in early_b:
        copy.start()
    for copy in late_a:
        copy.wait_recv()
    late2[column] = total_of(late1)
    late_b = stage(3, late2, column, column_member)
    for copy in late_b:
        copy.start()
    for copy in early_b:
        copy.wait_recv()

    def row(block, i):
        return jnp.concatenate([block[2 * i:2 * i + 1], block[2 * i + 1:2 * i + 2]], axis=1)

    def scale_of(mass):
        return 1.0 / jnp.sqrt(0.05 + mass / vertices)

    a, b = KEEP, TELEPORT
    early = total_of(early2)
    ff, f1, g11, ww2, wf2 = (row(early, i) for i in range(5))
    s1 = scale_of(a * a * g11 + 2 * a * b * f1 + b * b * ff)
    c = a * s1
    s2 = scale_of(c * c * ww2 + 2 * b * c * wf2 + b * b * ff)
    c3 = a * a * s1 * s2
    c1 = a * b * s2

    def blend(r, _):
        last[r] = c3 * last[r] + c1 * u1[r] + b * wide_f(r)
        return 0

    lax.fori_loop(0, NB, blend, 0)
    for copy in late_b:
        copy.wait_recv()
    ww3, w13, wf3 = (row(total_of(late2), i) for i in range(3))
    s3 = scale_of(
        c3 * c3 * ww3 + c1 * c1 * g11 + b * b * ff
        + 2 * c3 * (c1 * w13 + b * wf3) + 2 * b * c1 * f1
    )

    def finish(r, _):
        out[r] = (last[r] * s3).astype(jnp.bfloat16)
        return 0

    lax.fori_loop(0, NB, finish, 0)

    for step in range(ITERS):
        for j in range(SLOTS):
            for o in range(PEERS):
                halo_copy(step, o, j).wait_send()
    for copy in early_a + early_b + late_a + late_b:
        copy.wait_send()


def local(features, tile_values, tile_cols, halo_rows):
    classes = features.shape[1]
    rows = (NB, TILE, classes)
    anywhere = pl.BlockSpec(memory_space=pltpu.HBM)
    table = pltpu.VMEM((2 * NB, TILE, classes), jnp.bfloat16)
    blocks = pltpu.VMEM(rows, jnp.bfloat16)
    wide = pltpu.VMEM(rows, jnp.float32)
    inputs = [
        pltpu.with_memory_space_constraint(v, pltpu.HBM)
        for v in (features.reshape(rows), tile_values, tile_cols, halo_rows)
    ]
    scores = pl.pallas_call(
        kernel,
        out_shape=jax.ShapeDtypeStruct(rows, jnp.bfloat16),
        in_specs=[anywhere] * 4,
        out_specs=pl.BlockSpec(memory_space=pltpu.VMEM),
        scratch_shapes=[
            pltpu.SMEM(tile_cols.shape, jnp.int32),
            pltpu.SMEM(halo_rows.shape, jnp.int32),
            blocks,
            pltpu.VMEM(tile_values.shape, jnp.bfloat16),
            table, table, table,
            blocks, blocks, blocks,
            wide, wide, wide,
            pltpu.VMEM((8, 8, classes), jnp.float32),
            pltpu.VMEM((16, 10, HALF), jnp.float32),
            pltpu.VMEM((16, 10, HALF), jnp.float32),
            pltpu.VMEM((16, 6, HALF), jnp.float32),
            pltpu.VMEM((16, 6, HALF), jnp.float32),
            pltpu.SemaphoreType.DMA((5,)),
            pltpu.SemaphoreType.DMA((ITERS, NB)),
            pltpu.SemaphoreType.DMA((ITERS, NB)),
            pltpu.SemaphoreType.DMA((4, 15)),
            pltpu.SemaphoreType.DMA((4, 15)),
        ],
        compiler_params=pltpu.CompilerParams(
            collective_id=0, has_side_effects=True, vmem_limit_bytes=40 * 1024 * 1024
        ),
        name="propagate",
    )(*inputs)
    return scores.reshape(features.shape)


def solution(mesh):
    return jax.shard_map(
        local,
        mesh=mesh,
        in_specs=(
            P(("vp", "rep"), None),
            P(("vp", "rep"), None, None),
            P(("vp", "rep")),
            P(("vp", "rep"), None, None),
        ),
        out_specs=P(("vp", "rep"), None),
        check_vma=False,
    )
```

```python
import jax
import jax.numpy as jnp
from jax import lax
from jax.experimental import pallas as pl
from jax.experimental.pallas import tpu as pltpu
from jax.sharding import PartitionSpec as P

ITERS = 3
TILE = 128
NB = 16
SLOTS = 4
PEERS = 4
KEEP, TELEPORT = 0.9, 0.1
MESH = pl.DeviceIdType.MESH
HALF = 128


def kernel(
    feat_hbm, tiles_hbm, cols_hbm, halo_hbm, out,
    cols, halo, fbuf, tiles, tab0a, tab0b, tab1a, tab1b, tab2a, tab2b,
    snd0a, snd0b, snd1a, snd1b, snd2a, snd2b, u1, u2, last,
    gram, early1, early2, late1, late2,
    load_sem, halo_send, halo_recv, ar_send, ar_recv,
):
    vp, rep = lax.axis_index("vp"), lax.axis_index("rep")
    nvp, nrep = lax.axis_size("vp"), lax.axis_size("rep")
    shards = nvp * nrep
    me = vp * nrep + rep
    vertices = shards * NB * TILE
    plane = vp // 16 * nrep + rep
    column = vp % 16

    def plane_member(i):
        return (i // nrep * 16 + vp % 16, i % nrep)

    def column_member(i):
        return (vp // 16 * 16 + i, rep)

    core = vp % 2

    def peer(o):
        shift = (1 - o % 2 * 2) * (1 + o // 2 * 3)
        d = lax.rem(me + shift + shards, shards)
        return (d // nrep, d % nrep)

    leading, trailing, across, staying = 1 - core, core, 3 - core, 2 + core

    low, high = pl.ds(0, HALF), pl.ds(HALF, HALF)
    loads = [
        pltpu.make_async_copy(halo_hbm, halo, load_sem.at[0]),
        pltpu.make_async_copy(feat_hbm, fbuf, load_sem.at[1]),
        pltpu.make_async_copy(cols_hbm, cols, load_sem.at[2]),
        pltpu.make_async_copy(feat_hbm.at[:, :, low], tab0a.at[pl.ds(0, NB)], load_sem.at[3]),
        pltpu.make_async_copy(feat_hbm.at[:, :, high], tab0b.at[pl.ds(0, NB)], load_sem.at[4]),
        pltpu.make_async_copy(tiles_hbm, tiles, load_sem.at[5]),
    ]
    for copy in loads:
        copy.start()

    barrier = pltpu.get_barrier_semaphore()
    for o in range(PEERS):
        pl.semaphore_signal(barrier, inc=1, device_id=peer(o), device_id_type=MESH)
    for k in range(1, 16):
        pl.semaphore_signal(
            barrier, inc=1, device_id=plane_member((plane + k) % 16), device_id_type=MESH)
        pl.semaphore_signal(
            barrier, inc=1, device_id=column_member((column + k) % 16), device_id_type=MESH)
    gram[...] = jnp.zeros_like(gram)

    snd = ((snd0a, snd0b), (snd1a, snd1b), (snd2a, snd2b))
    tab = ((tab0a, tab0b), (tab1a, tab1b), (tab2a, tab2b))

    def halo_copy(step, half, o):
        return pltpu.make_async_remote_copy(
            src_ref=snd[step][half].at[pl.ds(o * SLOTS, SLOTS)],
            dst_ref=tab[step][half].at[pl.ds(NB + o * SLOTS, SLOTS)],
            send_sem=halo_send.at[step * 2 + half, o],
            recv_sem=halo_recv.at[step * 2 + half, o],
            device_id=peer(o),
            device_id_type=MESH,
        )

    def row_block(halves, r):
        total = None
        for p in range(NB // 2):
            pair = (r * NB + 2 * p, r * NB + 2 * p + 1)
            lhs = jnp.concatenate([tiles[t] for t in pair], axis=1)
            rhs = jnp.concatenate(
                [jnp.concatenate([h[cols[t]] for h in halves], axis=1) for t in pair], axis=0)
            term = jnp.dot(lhs, rhs, preferred_element_type=jnp.float32)
            total = term if total is None else total + term
        return total

    def fold(x):
        return jnp.sum(x.reshape(NB, 8, x.shape[-1]), axis=0)

    loads[0].wait()
    loads[1].wait()
    for o in range(PEERS):
        for j in range(SLOTS):
            block = fbuf[halo[0, o, j]]
            snd0a[o * SLOTS + j] = block[:, :HALF]
            snd0b[o * SLOTS + j] = block[:, HALF:]
    pl.semaphore_wait(barrier, PEERS + 30)
    for half in range(2):
        for o in (leading, trailing, across, staying):
            halo_copy(0, half, o).start()
    for copy in loads[2:]:
        copy.wait()

    def wait_halo(step, half):
        for o in range(PEERS):
            halo_copy(step, half, o).wait_recv()

    def send_pass(step, half):
        def body(g, _):
            o = g // 2 * 2 + (1 - core) + g % 2 * (2 * core - 1)
            for j in range(SLOTS):
                u = row_block((tab[step - 1][half],), halo[0, o, j])
                snd[step][half][o * SLOTS + j] = u.astype(jnp.bfloat16)
            halo_copy(step, half, o).start()
            return 0

        lax.fori_loop(0, PEERS, body, 0)

    def each_block(work):
        def body(q, _):
            for part in range(4):
                work(q * 4 + part)
            return 0

        lax.fori_loop(0, NB // 4, body, 0)

    def wide_f(r):
        return fbuf[r].astype(jnp.float32)

    def own_first(r):
        u = row_block(tab[0], r)
        u1[r] = u
        tab1a[r] = u[:, :HALF].astype(jnp.bfloat16)
        tab1b[r] = u[:, HALF:].astype(jnp.bfloat16)
        f = wide_f(r)
        gram[0] += fold(f * f)
        gram[1] += fold(f * u)
        gram[2] += fold(u * u)

    def own_second(r):
        u = row_block(tab[1], r)
        u2[r] = u
        tab2a[r] = u[:, :HALF].astype(jnp.bfloat16)
        tab2b[r] = u[:, HALF:].astype(jnp.bfloat16)
        w = KEEP * u + TELEPORT * u1[r]
        gram[3] += fold(w * w)
        gram[4] += fold(w * wide_f(r))

    def own_third(r):
        w = KEEP * row_block(tab[2], r) + TELEPORT * u2[r]
        last[r] = w
        gram[5] += fold(w * w)
        gram[6] += fold(w * u1[r])
        gram[7] += fold(w * wide_f(r))

    def pack(buf, mine, first, count):
        for i in range(count):
            row = jnp.sum(gram[first + i], axis=0, keepdims=True)
            for h in range(2):
                buf[mine, pl.ds(2 * i + h, 1), :] = row[:, h * HALF:(h + 1) * HALF]

    def stage(number, buf, mine, member):
        copies = []
        for k in range(1, 16):
            copies.append(pltpu.make_async_remote_copy(
                src_ref=buf.at[mine],
                dst_ref=buf.at[mine],
                send_sem=ar_send.at[number, k - 1],
                recv_sem=ar_recv.at[number, k - 1],
                device_id=member((mine + k) % 16),
                device_id_type=MESH,
            ))
        return copies

    def total_of(buf):
        total = buf[0]
        for i in range(1, 16):
            total = total + buf[i]
        return total

    for half in range(2):
        wait_halo(0, half)
        send_pass(1, half)
    each_block(own_first)
    for half in range(2):
        wait_halo(1, half)
        send_pass(2, half)
    each_block(own_second)
    pack(early1, plane, 0, 5)
    early_a = stage(0, early1, plane, plane_member)
    for copy in early_a:
        copy.start()
    wait_halo(2, 0)
    wait_halo(2, 1)
    each_block(own_third)
    pack(late1, plane, 5, 3)
    late_a = stage(2, late1, plane, plane_member)
    for copy in late_a:
        copy.start()
    for copy in early_a:
        copy.wait_recv()
    early2[column] = total_of(early1)
    early_b = stage(1, early2, column, column_member)
    for copy in early_b:
        copy.start()
    for copy in late_a:
        copy.wait_recv()
    late2[column] = total_of(late1)
    late_b = stage(3, late2, column, column_member)
    for copy in late_b:
        copy.start()
    for copy in early_b:
        copy.wait_recv()

    def row(block, i):
        return jnp.concatenate([block[2 * i:2 * i + 1], block[2 * i + 1:2 * i + 2]], axis=1)

    def scale_of(mass):
        return 1.0 / jnp.sqrt(0.05 + mass / vertices)

    a, b = KEEP, TELEPORT
    early = total_of(early2)
    ff, f1, g11, ww2, wf2 = (row(early, i) for i in range(5))
    s1 = scale_of(a * a * g11 + 2 * a * b * f1 + b * b * ff)
    c = a * s1
    s2 = scale_of(c * c * ww2 + 2 * b * c * wf2 + b * b * ff)
    c3 = a * a * s1 * s2
    c1 = a * b * s2

    def blend(r, _):
        last[r] = c3 * last[r] + c1 * u1[r] + b * wide_f(r)
        return 0

    lax.fori_loop(0, NB, blend, 0)
    for copy in late_b:
        copy.wait_recv()
    ww3, w13, wf3 = (row(total_of(late2), i) for i in range(3))
    s3 = scale_of(
        c3 * c3 * ww3 + c1 * c1 * g11 + b * b * ff
        + 2 * c3 * (c1 * w13 + b * wf3) + 2 * b * c1 * f1
    )

    def finish(r, _):
        out[r] = (last[r] * s3).astype(jnp.bfloat16)
        return 0

    lax.fori_loop(0, NB, finish, 0)

    for step in range(ITERS):
        for half in range(2):
            for o in range(PEERS):
                halo_copy(step, half, o).wait_send()
    for copy in early_a + early_b + late_a + late_b:
        copy.wait_send()


def local(features, tile_values, tile_cols, halo_rows):
    classes = features.shape[1]
    rows = (NB, TILE, classes)
    anywhere = pl.BlockSpec(memory_space=pltpu.HBM)
    table = pltpu.VMEM((2 * NB, TILE, HALF), jnp.bfloat16)
    parcels = pltpu.VMEM((NB, TILE, HALF), jnp.bfloat16)
    blocks = pltpu.VMEM(rows, jnp.bfloat16)
    wide = pltpu.VMEM(rows, jnp.float32)
    inputs = [
        pltpu.with_memory_space_constraint(v, pltpu.HBM)
        for v in (features.reshape(rows), tile_values, tile_cols, halo_rows)
    ]
    scores = pl.pallas_call(
        kernel,
        out_shape=jax.ShapeDtypeStruct(rows, jnp.bfloat16),
        in_specs=[anywhere] * 4,
        out_specs=pl.BlockSpec(memory_space=pltpu.VMEM),
        scratch_shapes=[
            pltpu.SMEM(tile_cols.shape, jnp.int32),
            pltpu.SMEM(halo_rows.shape, jnp.int32),
            blocks,
            pltpu.VMEM(tile_values.shape, jnp.bfloat16),
            *[table] * 6,
            *[parcels] * 6,
            wide, wide, wide,
            pltpu.VMEM((8, 8, classes), jnp.float32),
            pltpu.VMEM((16, 10, HALF), jnp.float32),
            pltpu.VMEM((16, 10, HALF), jnp.float32),
            pltpu.VMEM((16, 6, HALF), jnp.float32),
            pltpu.VMEM((16, 6, HALF), jnp.float32),
            pltpu.SemaphoreType.DMA((6,)),
            pltpu.SemaphoreType.DMA((2 * ITERS, PEERS)),
            pltpu.SemaphoreType.DMA((2 * ITERS, PEERS)),
            pltpu.SemaphoreType.DMA((4, 15)),
            pltpu.SemaphoreType.DMA((4, 15)),
        ],
        compiler_params=pltpu.CompilerParams(
            collective_id=0, has_side_effects=True, vmem_limit_bytes=40 * 1024 * 1024
        ),
        name="propagate",
    )(*inputs)
    return scores.reshape(features.shape)


def solution(mesh):
    return jax.shard_map(
        local,
        mesh=mesh,
        in_specs=(
            P(("vp", "rep"), None),
            P(("vp", "rep"), None, None),
            P(("vp", "rep")),
            P(("vp", "rep"), None, None),
        ),
        out_specs=P(("vp", "rep"), None),
        check_vma=False,
    )
```
